8 devices in a mesh: dp: 1 (over z), emb: 2 (over y), head: 4 (over x, core).
Axes of the slice: x: 2, y: 2, z: 1, core: 2. Of those that a mesh axis runs over, the one named last changes fastest.
Arguments:
- hidden: bfloat16 [16, 512, 7168], P('dp', None, 'emb')
- g_in: bfloat16 [7168], P('emb')
- w_dq: bfloat16 [7168, 1536], P('emb', 'head')
- g_q: bfloat16 [1536], P('head')
- w_dkv: bfloat16 [7168, 512], P('emb', 'head')
- g_kv: bfloat16 [512], P('head')
- w_kr: bfloat16 [7168, 64], P('emb')
- w_uq: bfloat16 [1536, 64, 192], P(None, 'head')
- w_uk: bfloat16 [512, 64, 128], P(None, 'head')
- w_uv: bfloat16 [512, 64, 128], P(None, 'head')
- w_o: bfloat16 [64, 128, 7168], P('head', None, 'emb')
Outputs:
- output 1: bfloat16 [16, 512, 7168], P('dp', None, 'emb')
- output 2: bfloat16 [16, 512, 512], P('dp', None, 'head')
- output 3: bfloat16 [16, 512, 64], P('dp')
All inputs are finite; a program needn't handle non-finite values.
Results may differ from the reference program's by a relative error of at most 0.0181088.
Values are sent between devices in bfloat16 or wider.
A program may use at most 1 GiB of HBM per device.

```python
import math
import jax
import jax.numpy as jnp
from jax import lax

BATCH = 16
SEQ = 512
D = 7168
HEADS = 64
Q_LORA = 1536
KV_LORA = 512
NOPE = 128
ROPE = 64
VDIM = 128

QK_DIM = NOPE + ROPE
HALF_ROPE = ROPE // 2
Q_BLOCK = min(SEQ, 128)
BLOCKS_PER_SEQ = SEQ // Q_BLOCK
NUM_BLOCKS = BATCH * BLOCKS_PER_SEQ
ROPE_BASE = 10000.0
NORM_EPS = 1.0e-6
MSCALE = 0.1 * math.log(40.0) + 1.0
SOFTMAX_SCALE = MSCALE * MSCALE / math.sqrt(QK_DIM)


def setup_inputs(seed: int = 0, part: int = 0) -> dict:
    key_list = jax.random.split(jax.random.key(seed), 10)
    part_key = jax.random.fold_in(jax.random.key(seed + 1), part)

    def make_gain(sub_key, count):
        return jax.random.uniform(sub_key, (count,), jnp.float32, 0.5, 1.5).astype(jnp.bfloat16)

    def weight(sub_key, arr_shape, fan_in):
        return (jax.random.normal(sub_key, arr_shape, jnp.float32) * fan_in ** -0.5).astype(jnp.bfloat16)

    hidden = 0.5 * jax.random.normal(part_key, (BATCH, SEQ, D), jnp.float32)
    return {
        "hidden": hidden.astype(jnp.bfloat16),
        "g_in": make_gain(key_list[0], D),
        "w_dq": weight(key_list[1], (D, Q_LORA), D),
        "g_q": make_gain(key_list[2], Q_LORA),
        "w_dkv": weight(key_list[3], (D, KV_LORA), D),
        "g_kv": make_gain(key_list[4], KV_LORA),
        "w_kr": weight(key_list[5], (D, ROPE), D),
        "w_uq": weight(key_list[6], (Q_LORA, HEADS, QK_DIM), Q_LORA),
        "w_uk": weight(key_list[7], (KV_LORA, HEADS, NOPE), KV_LORA),
        "w_uv": weight(key_list[8], (KV_LORA, HEADS, VDIM), KV_LORA),
        "w_o": weight(key_list[9], (HEADS, VDIM, D), HEADS * VDIM),
    }


def rms_norm(values, gain_vec):
    wide_vals = values.astype(jnp.float32)
    mean_sq = jnp.mean(wide_vals * wide_vals, axis=-1, keepdims=True)
    return (wide_vals * lax.rsqrt(mean_sq + NORM_EPS) * gain_vec.astype(jnp.float32)).astype(jnp.bfloat16)


def rope_tables():
    inv_freq = ROPE_BASE ** (-2.0 * jnp.arange(HALF_ROPE, dtype=jnp.float32) / ROPE)
    angles = jnp.arange(SEQ, dtype=jnp.float32)[:, None] * inv_freq[None, :]
    return jnp.cos(angles), jnp.sin(angles)


def rotate(values, cos_t, sin_t):
    front_half = values[..., :HALF_ROPE]
    back_half = values[..., HALF_ROPE:]
    return jnp.concatenate([front_half * cos_t - back_half * sin_t, front_half * sin_t + back_half * cos_t], axis=-1)


def reference(hidden, g_in, w_dq, g_q, w_dkv, g_kv, w_kr, w_uq, w_uk, w_uv, w_o):
    tokens = rms_norm(hidden, g_in).reshape(BATCH * SEQ, D)
    c_q = jnp.dot(tokens, w_dq, preferred_element_type=jnp.float32).astype(jnp.bfloat16)
    c_kv = jnp.dot(tokens, w_dkv, preferred_element_type=jnp.float32).astype(jnp.bfloat16)
    k_raw = jnp.dot(tokens, w_kr, preferred_element_type=jnp.float32).astype(jnp.bfloat16)
    cq_norm = rms_norm(c_q, g_q)
    ckv_norm = rms_norm(c_kv, g_kv)
    cos_t, sin_t = rope_tables()
    k_pe = rotate(k_raw.reshape(BATCH, SEQ, ROPE).astype(jnp.float32), cos_t, sin_t).astype(jnp.bfloat16)
    q_all = jnp.dot(cq_norm, w_uq.reshape(Q_LORA, HEADS * QK_DIM), preferred_element_type=jnp.float32)
    q_all = q_all.astype(jnp.bfloat16).reshape(BATCH, SEQ, HEADS, QK_DIM)
    q_nope = q_all[..., :NOPE]
    q_pe = rotate(q_all[..., NOPE:].astype(jnp.float32), cos_t[:, None, :], sin_t[:, None, :]).astype(jnp.bfloat16)
    k_nope = jnp.dot(ckv_norm, w_uk.reshape(KV_LORA, HEADS * NOPE), preferred_element_type=jnp.float32)
    k_nope = k_nope.astype(jnp.bfloat16).reshape(BATCH, SEQ, HEADS, NOPE)
    v_heads = jnp.dot(ckv_norm, w_uv.reshape(KV_LORA, HEADS * VDIM), preferred_element_type=jnp.float32)
    v_heads = v_heads.astype(jnp.bfloat16).reshape(BATCH, SEQ, HEADS, VDIM)
    key_pos = jnp.arange(SEQ)

    def attend_block(blk_idx):
        seq_idx = blk_idx // BLOCKS_PER_SEQ
        q_start = (blk_idx % BLOCKS_PER_SEQ) * Q_BLOCK
        qn_seq = lax.dynamic_index_in_dim(q_nope, seq_idx, 0, keepdims=False)
        qp_seq = lax.dynamic_index_in_dim(q_pe, seq_idx, 0, keepdims=False)
        qn_blk = lax.dynamic_slice_in_dim(qn_seq, q_start, Q_BLOCK, 0).astype(jnp.float32)
        qp_blk = lax.dynamic_slice_in_dim(qp_seq, q_start, Q_BLOCK, 0).astype(jnp.float32)
        kn_seq = lax.dynamic_index_in_dim(k_nope, seq_idx, 0, keepdims=False).astype(jnp.float32)
        kp_seq = lax.dynamic_index_in_dim(k_pe, seq_idx, 0, keepdims=False).astype(jnp.float32)
        v_seq = lax.dynamic_index_in_dim(v_heads, seq_idx, 0, keepdims=False).astype(jnp.float32)
        scores = jnp.einsum("qhd,khd->hqk", qn_blk, kn_seq) + jnp.einsum("qhr,kr->hqk", qp_blk, kp_seq)
        q_pos = q_start + jnp.arange(Q_BLOCK)
        allowed = key_pos[None, :] <= q_pos[:, None]
        scores = jnp.where(allowed[None, :, :], scores * SOFTMAX_SCALE, -jnp.inf)
        attn_prob = jax.nn.softmax(scores, axis=-1).astype(jnp.bfloat16).astype(jnp.float32)
        return jnp.einsum("hqk,khv->qhv", attn_prob, v_seq).astype(jnp.bfloat16)

    context = lax.map(attend_block, jnp.arange(NUM_BLOCKS)).reshape(BATCH * SEQ, HEADS * VDIM)
    attn_sum = jnp.dot(context, w_o.reshape(HEADS * VDIM, D), preferred_element_type=jnp.float32)
    result = (hidden.astype(jnp.float32) + attn_sum.reshape(BATCH, SEQ, D)).astype(jnp.bfloat16)
    return (result, ckv_norm.reshape(BATCH, SEQ, KV_LORA), k_pe)
```

```python
import math
import jax
import jax.numpy as jnp
from jax import lax
from jax.experimental import pallas as pl
from jax.experimental.pallas import tpu as pltpu
from jax.sharding import PartitionSpec as P

ROPE_BASE = 10000.0
NORM_EPS = 1.0e-6
MSCALE = 0.1 * math.log(40.0) + 1.0
BF16 = jnp.bfloat16
F32 = jnp.float32


SIBLING = [(0, 1), (1, 0), (2, 3), (3, 2)]
ACROSS = [(0, 2), (2, 0), (1, 3), (3, 1)]
EMB_SWAP = [(0, 1), (1, 0)]

FIRST = 2
DOWNS = {0: ((2, 2),), 2: ((4, 4),)}
PIECES = {7: ((0, 256), (256, 512))}
ROWS = 256


def after(value, *deps):
    return lax.optimization_barrier((value,) + deps)[0]


def rope_tables(seq_len, rope_dim):
    half_dim = rope_dim // 2
    inv_freq = ROPE_BASE ** (-2.0 * jnp.arange(half_dim, dtype=F32) / rope_dim)
    angles = jnp.arange(seq_len, dtype=F32)[:, None] * inv_freq[None, :]
    cos_t, sin_t = jnp.cos(angles), jnp.sin(angles)
    return jnp.concatenate([cos_t] * 4, axis=1), jnp.concatenate([-sin_t, -sin_t, sin_t, sin_t], axis=1)


def down_kernel(offs_ref, h_ref, rstd_ref, g_ref, *rest):
    pieces, out_ref, w_all = rest[:-2], rest[-2], rest[-1]

    @pl.when(pl.program_id(0) == 0)
    def _():
        for k, ref in enumerate(pieces):
            off = pl.multiple_of(offs_ref[k + 1], 128)
            w_all[:, pl.ds(off, ref.shape[1])] = ref[...]

    hn = (h_ref[0].astype(F32) * rstd_ref[0] * g_ref[...]).astype(BF16)
    out_ref[...] = jnp.dot(hn, w_all[...], preferred_element_type=F32).astype(BF16)


def down(hidden, rstd, g_in, first, n, core_base, pieces, offsets):
    seq, width = hidden.shape[1:]
    tiles = seq // ROWS
    total = sum(p.shape[1] for p in pieces)
    offs = jnp.stack([core_base + first] + [jnp.asarray(o, jnp.int32) for o in offsets]).astype(jnp.int32)
    whole = lambda p: pl.BlockSpec(p.shape, lambda t, o: (0, 0), pipeline_mode=pl.Buffered(1))
    return pl.pallas_call(
        down_kernel,
        grid_spec=pltpu.PrefetchScalarGridSpec(
            num_scalar_prefetch=1,
            grid=(n * tiles,),
            in_specs=[
                pl.BlockSpec((1, ROWS, width), lambda t, o: (o[0] + t // tiles, t % tiles, 0)),
                pl.BlockSpec((1, ROWS, 1), lambda t, o: (first + t // tiles, t % tiles, 0)),
                whole(g_in),
            ] + [whole(p) for p in pieces],
            out_specs=pl.BlockSpec((ROWS, total), lambda t, o: (t, 0)),
            scratch_shapes=[pltpu.VMEM((width, total), BF16)],
        ),
        out_shape=jax.ShapeDtypeStruct((n * seq, total), BF16),
        compiler_params=pltpu.CompilerParams(dimension_semantics=("arbitrary",)),
        cost_estimate=pl.CostEstimate(flops=2 * n * seq * width * total, bytes_accessed=2 * n * seq * width + 2 * width * total, transcendentals=0),
        name="down",
    )(offs, hidden, rstd, g_in, *pieces)


def block_kernel(scale, split, side_ref, *refs):
    n_in = 3 if split else 2
    ins = refs[:n_in]
    gq_ref, gkv_ref, cos_ref, sin_ref, wq_ref, wk_ref, wv_ref, wo_a_ref, wo_b_ref = refs[n_in:n_in + 9]
    part_ref, ckv_ref, kk_ref, cq_ref, kpe_ref, ctx_ref = refs[n_in + 9:]
    step = pl.program_id(0)
    seq, q_lora = cq_ref.shape
    kv_lora = ckv_ref.shape[1]
    heads = wq_ref.shape[0]
    wide = heads * 128
    steps = ctx_ref.shape[1] // wide
    blk = 256

    def norm(vals, gain):
        mean_sq = jnp.mean(vals * vals, axis=-1, keepdims=True)
        return (vals * lax.rsqrt(mean_sq + NORM_EPS) * gain).astype(BF16)

    @pl.when(step == 0)
    def _():
        @pl.loop(0, seq // 128)
        def _(c):
            rows = pl.ds(pl.multiple_of(c * 128, 128), 128)

            def summed(a_ref, b_ref, lo, hi):
                return (a_ref[rows, lo:hi].astype(F32) + b_ref[rows, lo:hi].astype(F32)).astype(BF16).astype(F32)

            if split:
                first = side_ref[0] == 0
                qh, kh = q_lora // 2, kv_lora // 2

                def both(lo, hi):
                    own, far = ins[0][rows, lo:hi].astype(F32), ins[1][rows, lo:hi].astype(F32)
                    return jnp.concatenate([jnp.where(first, own, far), jnp.where(first, far, own)], axis=1)

                cq, ckv, kr = both(0, qh), both(qh, qh + kh), ins[2][rows].astype(F32)
            else:
                cq, ckv = summed(ins[0], ins[1], 0, q_lora), summed(ins[0], ins[1], q_lora, q_lora + kv_lora)
                kr = summed(ins[0], ins[1], q_lora + kv_lora, q_lora + kv_lora + 128)
            cq_ref[rows] = norm(cq, gq_ref[...])
            ckv_ref[rows] = norm(ckv, gkv_ref[...])
            kk = kr * cos_ref[rows] + pltpu.roll(kr, 64, 1) * sin_ref[rows]
            odd = (lax.broadcasted_iota(jnp.int32, kk.shape, 1) // 32) % 2 == 1
            kk_ref[rows] = kk.astype(BF16)
            kpe_ref[0, rows] = jnp.where(odd, 0.0, kk).astype(BF16)
            kpe_ref[1, rows] = jnp.where(odd, kk, 0.0).astype(BF16)

    def nt(a, b):
        return lax.dot_general(a, b, (((1,), (1,)), ((), ())), preferred_element_type=F32)

    @pl.when(step < steps)
    def _():
        cq, ckv = cq_ref[...], ckv_ref[...]
        qn = nt(cq, wq_ref[:, :128].reshape(wide, q_lora)).astype(BF16)
        qps = []
        for pair in range(heads // 2):
            a, b = 2 * pair, 2 * pair + 1
            wr = jnp.concatenate([wq_ref[a, 128:160], wq_ref[b, 128:160], wq_ref[a, 160:192], wq_ref[b, 160:192]], axis=0)
            qr = nt(cq, wr).astype(BF16).astype(F32)
            qps.append((qr * cos_ref[...] + pltpu.roll(qr, 64, 1) * sin_ref[...]).astype(BF16))
        kn = jnp.dot(ckv, wk_ref[...], preferred_element_type=F32).astype(BF16)
        val = jnp.dot(ckv, wv_ref[...], preferred_element_type=F32).astype(BF16)
        row = lax.broadcasted_iota(jnp.int32, (blk, blk), 0)
        col = lax.broadcasted_iota(jnp.int32, (blk, blk), 1)
        allowed = col <= row
        items = [(hh, qb) for hh in range(heads) for qb in range(seq // blk)]

        def score(hh, qb):
            cols, rows, end = slice(hh * 128, hh * 128 + 128), slice(qb * blk, (qb + 1) * blk), (qb + 1) * blk
            key = jnp.concatenate([kn[:end, cols], kpe_ref[hh % 2, :end]], axis=1)
            q = jnp.concatenate([qn[rows, cols], qps[hh // 2][rows]], axis=1)
            s = nt(q, key)
            diag = jnp.where(allowed, s[:, end - blk:], -jnp.inf)
            return diag if qb == 0 else jnp.concatenate([s[:, :end - blk], diag], axis=1)

        def softmax(s):
            top = jnp.max(s, axis=1, keepdims=True)
            e = jnp.exp2((s - top) * (scale * math.log2(math.e)))
            return (e * (1.0 / jnp.sum(e, axis=1, keepdims=True))).astype(BF16)

        scores = [score(*it) for it in items]
        probs = [softmax(s) for s in scores]
        for p, (hh, qb) in zip(probs, items):
            rows, end = slice(qb * blk, (qb + 1) * blk), (qb + 1) * blk
            o = jnp.dot(p, val[:end, hh * 128:hh * 128 + 128], preferred_element_type=F32).astype(BF16)
            ctx_ref[rows, pl.ds(pl.multiple_of(step * wide + hh * 128, 128), 128)] = o

    @pl.when(step >= steps)
    def _():
        depth = wo_a_ref.shape[0]
        out = jnp.dot(ctx_ref[:, :depth], wo_a_ref[...], preferred_element_type=F32)
        out += jnp.dot(ctx_ref[:, depth:], wo_b_ref[...], preferred_element_type=F32)
        part_ref[...] = out.astype(BF16)


def head_block(ins, at, side, gq, gkv, cos_p, sin_p, wq, wkv, wo_a, wo_b, scale):
    seq = cos_p.shape[0]
    n_heads, qk, q_lora = wq.shape
    kv_lora, depth, width = wkv.shape[0], wo_a.shape[0], wo_a.shape[1]
    heads, wide = 4, 512
    steps, out_steps = n_heads // heads, width // wide
    once = pl.Buffered(1)
    hd = lambda j: jnp.minimum(j, steps - 1)
    oc = lambda j: jnp.maximum(j - steps, 0)
    const = lambda shape: pl.BlockSpec(shape, lambda j, o: (0,) * len(shape), pipeline_mode=once)
    return pl.pallas_call(
        lambda *refs: block_kernel(scale, len(ins) == 3, *refs),
        grid_spec=pltpu.PrefetchScalarGridSpec(
            num_scalar_prefetch=1,
            grid=(steps + out_steps,),
            in_specs=[pl.BlockSpec((seq, a.shape[1]), lambda j, o, r=r: (r, 0), pipeline_mode=once) for a, r in zip(ins, at)] + [
                const((1, q_lora)), const((1, kv_lora)), const((seq, 128)), const((seq, 128)),
                pl.BlockSpec((heads, qk, q_lora), lambda j, o: (hd(j), 0, 0)),
                pl.BlockSpec((kv_lora, wide), lambda j, o: (0, hd(j))),
                pl.BlockSpec((kv_lora, wide), lambda j, o: (0, steps + hd(j))),
                pl.BlockSpec((depth, wide), lambda j, o: (0, oc(j))),
                pl.BlockSpec((depth, wide), lambda j, o: (0, oc(j))),
            ],
            out_specs=[
                pl.BlockSpec((seq, wide), lambda j, o: (0, oc(j))),
                pl.BlockSpec((seq, kv_lora), lambda j, o: (0, 0)),
                pl.BlockSpec((seq, 128), lambda j, o: (0, 0)),
            ],
            scratch_shapes=[pltpu.VMEM((seq, q_lora), BF16), pltpu.VMEM((2, seq, 128), BF16), pltpu.VMEM((seq, n_heads * 128), BF16)],
        ),
        out_shape=[jax.ShapeDtypeStruct((seq, width), BF16), jax.ShapeDtypeStruct((seq, kv_lora), BF16), jax.ShapeDtypeStruct((seq, 128), BF16)],
        compiler_params=pltpu.CompilerParams(dimension_semantics=("arbitrary",), vmem_limit_bytes=60 * 2**20),
        cost_estimate=pl.CostEstimate(flops=45 * 10**9, bytes_accessed=64 * 10**6, transcendentals=n_heads * seq * seq),
        name="block",
    )(side, *ins, gq, gkv, cos_p, sin_p, wq, wkv, wkv, wo_a, wo_b)


def blank(shape, dtype):
    return pl.pallas_call(lambda o_ref: None, out_shape=jax.ShapeDtypeStruct(shape, dtype), out_specs=pl.BlockSpec(memory_space=pl.ANY), name="blank")()


def solution(mesh):
    emb_count = mesh.shape["emb"]
    in_specs = (P("dp", None, "emb"), P("emb"), P("emb", "head"), P("head"), P("emb", "head"), P("head"), P("emb", None), P(None, "head", None), P(None, "head", None), P(None, "head", None), P("head", None, "emb"))
    out_specs = (P("dp", None, "emb"), P("dp", None, "head"), P("dp", None, None))

    def swap(v):
        return lax.ppermute(v, "head", SIBLING)

    def cross(v):
        return lax.ppermute(v, "head", ACROSS)

    def emb_swap(v):
        return lax.ppermute(v, "emb", EMB_SWAP)

    def block(hidden, g_in, w_dq, g_q, w_dkv, g_kv, w_kr, w_uq, w_uk, w_uv, w_o):
        n_seq, seq, width = hidden.shape
        half = n_seq // 2
        own_heads = w_uk.shape[1]
        q_lora, kv_lora = w_uq.shape[0], w_uk.shape[0]
        q_blk, kv_blk = w_dq.shape[1], w_dkv.shape[1]
        rope = w_kr.shape[1]
        hr = rope // 2
        scale = MSCALE * MSCALE / math.sqrt(w_uq.shape[2])
        pos = lax.axis_index("head")
        core = lax.rem(pos, 2)
        side = lax.div(pos, 2)
        base = core * half

        far_q = cross(w_dq)
        near_q, near_kv = swap(w_dq), swap(w_dkv)
        sib_uq, sib_uk, sib_uv = swap(w_uq), swap(w_uk), swap(w_uv)
        sib_o = swap(w_o)

        cos_p, sin_p = rope_tables(seq, rope)
        w_kr2 = jnp.concatenate([w_kr[:, :hr], w_kr[:, :hr], w_kr[:, hr:], w_kr[:, hr:]], axis=1)
        gain = jnp.concatenate([g_q, g_kv])[None]
        far_gain = cross(gain)
        g_row = g_in.astype(F32)[None]

        h_wide = lax.dynamic_slice_in_dim(hidden, base, half, 0).astype(F32)
        sq = jnp.sum(h_wide * h_wide, axis=-1)
        sq = sq + emb_swap(sq)
        rstd = lax.rsqrt(sq / (width * emb_count) + NORM_EPS)[:, :, None]

        qh, kh = 2 * q_blk, 2 * kv_blk
        near_offs = [core * q_blk, (1 - core) * q_blk, qh + core * kv_blk, qh + (1 - core) * kv_blk]
        low_own = down(hidden, rstd, g_row, 0, FIRST, base, [w_dq, near_q, w_dkv, near_kv, w_kr2], near_offs + [qh + kh])

        def rows_of(low, r):
            return low[r * seq:(r + 1) * seq]

        own_in = [emb_swap(rows_of(low_own, r)) for r in range(FIRST)]

        w_uq, sib_uq = after((w_uq, sib_uq), low_own)
        flat = lambda w: w.reshape(kv_lora, own_heads * 128)
        wq_all = jnp.concatenate([w_uq.transpose(1, 2, 0), sib_uq.transpose(1, 2, 0)], axis=0)
        wkv_all = jnp.concatenate([flat(w_uk), flat(sib_uk), flat(w_uv), flat(sib_uv)], axis=1)
        wo_own, wo_sib = w_o.reshape(own_heads * 128, width), sib_o.reshape(own_heads * 128, width)

        lows = {}
        for r in range(FIRST):
            arrived_r = own_in[r] if r == 0 else after(own_in[r], lat)
            lat = (rows_of(low_own, r).astype(F32) + arrived_r.astype(F32)).astype(BF16)
            far_lat = cross(lat[:, :qh + kh])
            lows[r] = ((lat[:, :qh + kh], far_lat, lat[:, qh + kh:]), (0, 0, 0))
        far_kv = cross(after(w_dkv, lat))

        far_gain, far_q = after((far_gain, far_q), wq_all, wkv_all)
        gains = jnp.concatenate([gain, swap(gain), far_gain, swap(far_gain)], axis=0).astype(F32)
        gains = jnp.concatenate([lax.dynamic_slice_in_dim(gains, lax.bitwise_xor(pos, r), 1, 0) for r in range(4)], axis=0)
        gq_all = gains[:, :q_blk].reshape(1, q_lora)
        gkv_all = gains[:, q_blk:].reshape(1, kv_lora)
        diag_q = swap(far_q)
        every_offs = [lax.bitwise_xor(pos, r) * q_blk for r in range(4)] + [q_lora + lax.bitwise_xor(pos, r) * kv_blk for r in range(4)] + [q_lora + kv_lora]

        side_flag = side.astype(jnp.int32)[None]
        parts, arrived, ckvs, kks = [], {}, [], []
        last = wq_all
        result = blank(hidden.shape, BF16)

        def finish(i, lo, hi, dep):
            at = after(base, *dep)
            h_i = lax.dynamic_slice(hidden, (at + i, 0 * at + lo, 0 * at), (1, hi - lo, width)).astype(F32)
            total = parts[i][lo:hi].astype(F32) + arrived[i, lo].astype(F32)
            return (h_i + total[None]).astype(BF16)

        for i in range(half):
            gq_i = after(gq_all, last)
            ins, at = lows[i]
            part, ckv, kk = head_block(ins, at, side_flag, gq_i, gkv_all, cos_p, sin_p, wq_all, wkv_all, wo_own, wo_sib, scale)
            ckvs.append(ckv)
            kks.append(kk)
            parts.append(part)
            for lo, hi in PIECES.get(i, ((0, seq),)):
                arrived[i, lo] = cross(part[lo:hi])
            last = part
            if i == 0:
                far_kv = after(far_kv, part)
                diag_kv = swap(far_kv)
                every = [w_dq, near_q, far_q, diag_q, w_dkv, near_kv, far_kv, diag_kv, w_kr2]
            for first, n in DOWNS.get(i, ()):
                low = down(hidden, after(rstd, last), g_row, first, n, base, every, every_offs)
                last = low
                for r in range(n):
                    lows[first + r] = ((low, emb_swap(rows_of(low, r))), (r, 0))

        def spread(own, other):
            full = blank((n_seq,) + own.shape[1:], own.dtype)
            full = lax.dynamic_update_slice_in_dim(full, own, base, 0)
            return lax.dynamic_update_slice_in_dim(full, other, half - base, 0)

        ckv_own = jnp.concatenate(ckvs, axis=0).reshape(half, seq, kv_lora)
        kk = jnp.concatenate(kks, axis=0)
        kk = jnp.concatenate([kk[:, :hr], kk[:, 2 * hr:3 * hr]], axis=1).reshape(half, seq, rope)
        mine = lax.dynamic_slice_in_dim(ckv_own, pos * kv_blk, kv_blk, 2)
        theirs = lax.dynamic_slice_in_dim(ckv_own, lax.bitwise_xor(pos, 1) * kv_blk, kv_blk, 2)
        ckv_out, kpe_out = spread(mine, swap(theirs)), spread(kk, swap(kk))

        waiting = []

        def place(result):
            i, lo, other = waiting.pop(0)
            return lax.dynamic_update_slice(result, other, (half - base + i, 0 * base + lo, 0 * base))

        for i in range(half):
            for lo, hi in PIECES.get(i, ((0, seq),)):
                out_i = finish(i, lo, hi, (last,))
                waiting.append((i, lo, swap(out_i)))
                result = lax.dynamic_update_slice(result, out_i, (base + i, 0 * base + lo, 0 * base))
                if len(waiting) > 1:
                    result = place(result)
        result = place(result)
        return result, ckv_out, kpe_out

    return jax.shard_map(block, mesh=mesh, in_specs=in_specs, out_specs=out_specs, check_vma=False)
```

```python
import math
import jax
import jax.numpy as jnp
from jax import lax
from jax.experimental import pallas as pl
from jax.experimental.pallas import tpu as pltpu
from jax.sharding import PartitionSpec as P

ROPE_BASE = 10000.0
NORM_EPS = 1.0e-6
MSCALE = 0.1 * math.log(40.0) + 1.0
BF16 = jnp.bfloat16
F32 = jnp.float32


SIBLING = [(0, 1), (1, 0), (2, 3), (3, 2)]
ACROSS = [(0, 2), (2, 0), (1, 3), (3, 1)]
EMB_SWAP = [(0, 1), (1, 0)]

FIRST = 3
DOWNS = {1: ((3, 1),), 2: ((4, 1),), 3: ((5, 3),)}
PIECES = {0: ((0, 256), (256, 512)), 7: ((0, 384), (384, 512))}
ROWS = 256


def after(value, *deps):
    return lax.optimization_barrier((value,) + deps)[0]


def rope_tables(seq_len, rope_dim):
    half_dim = rope_dim // 2
    inv_freq = ROPE_BASE ** (-2.0 * jnp.arange(half_dim, dtype=F32) / rope_dim)
    angles = jnp.arange(seq_len, dtype=F32)[:, None] * inv_freq[None, :]
    cos_t, sin_t = jnp.cos(angles), jnp.sin(angles)
    return jnp.concatenate([cos_t] * 4, axis=1), jnp.concatenate([-sin_t, -sin_t, sin_t, sin_t], axis=1)


def down_kernel(offs_ref, h_ref, rstd_ref, g_ref, *rest):
    pieces, out_ref, w_all = rest[:-2], rest[-2], rest[-1]

    @pl.when(pl.program_id(0) == 0)
    def _():
        for k, ref in enumerate(pieces):
            off = pl.multiple_of(offs_ref[k + 1], 128)
            w_all[:, pl.ds(off, ref.shape[1])] = ref[...]

    hn = (h_ref[0].astype(F32) * rstd_ref[0] * g_ref[...]).astype(BF16)
    out_ref[...] = jnp.dot(hn, w_all[...], preferred_element_type=F32).astype(BF16)


def down(hidden, rstd, g_in, first, n, core_base, pieces, offsets):
    seq, width = hidden.shape[1:]
    tiles = seq // ROWS
    total = sum(p.shape[1] for p in pieces)
    offs = jnp.stack([core_base + first] + [jnp.asarray(o, jnp.int32) for o in offsets]).astype(jnp.int32)
    whole = lambda p: pl.BlockSpec(p.shape, lambda t, o: (0, 0), pipeline_mode=pl.Buffered(1))
    return pl.pallas_call(
        down_kernel,
        grid_spec=pltpu.PrefetchScalarGridSpec(
            num_scalar_prefetch=1,
            grid=(n * tiles,),
            in_specs=[
                pl.BlockSpec((1, ROWS, width), lambda t, o: (o[0] + t // tiles, t % tiles, 0)),
                pl.BlockSpec((1, ROWS, 1), lambda t, o: (first + t // tiles, t % tiles, 0)),
                whole(g_in),
            ] + [whole(p) for p in pieces],
            out_specs=pl.BlockSpec((ROWS, total), lambda t, o: (t, 0)),
            scratch_shapes=[pltpu.VMEM((width, total), BF16)],
        ),
        out_shape=jax.ShapeDtypeStruct((n * seq, total), BF16),
        compiler_params=pltpu.CompilerParams(dimension_semantics=("arbitrary",)),
        cost_estimate=pl.CostEstimate(flops=2 * n * seq * width * total, bytes_accessed=2 * n * seq * width + 2 * width * total, transcendentals=0),
        name="down",
    )(offs, hidden, rstd, g_in, *pieces)


def block_kernel(scale, mode, q_lo, side_ref, *refs):
    n_in = {"full": 2, "pair": 4, "sum": 3, "sum2": 6}[mode]
    ins = refs[:n_in]
    gq_ref, gkv_ref, cos_ref, sin_ref, wq_ref, wk_ref, wv_ref, wo_a_ref, wo_b_ref = refs[n_in:n_in + 9]
    part_ref, ckv_ref, kk_ref, cq_ref, kpe_ref, ctx_ref = refs[n_in + 9:]
    step = pl.program_id(0)
    q_rows, q_lora = cq_ref.shape
    seq, kv_lora = ckv_ref.shape
    heads = wq_ref.shape[0]
    wide = heads * 128
    steps = ctx_ref.shape[1] // wide
    blk = 256
    qh, kh = q_lora // 2, kv_lora // 2

    def norm(vals, gain):
        mean_sq = jnp.mean(vals * vals, axis=-1, keepdims=True)
        return (vals * lax.rsqrt(mean_sq + NORM_EPS) * gain).astype(BF16)

    def fill(group, start, count):
        @pl.loop(0, count // 128)
        def _(c):
            src = pl.ds(pl.multiple_of(c * 128, 128), 128)
            rows = pl.ds(pl.multiple_of(start + c * 128, 128), 128)

            def summed(a_ref, b_ref, lo, hi):
                return (a_ref[src, lo:hi].astype(F32) + b_ref[src, lo:hi].astype(F32)).astype(BF16).astype(F32)

            def halves(lo, hi):
                if mode == "pair":
                    own, far = summed(group[0], group[1], lo, hi), summed(group[2], group[3], lo, hi)
                else:
                    own, far = group[0][src, lo:hi].astype(F32), group[1][src, lo:hi].astype(F32)
                first = side_ref[0] == 0
                return jnp.concatenate([jnp.where(first, own, far), jnp.where(first, far, own)], axis=1)

            if mode == "full":
                ckv, kr = summed(group[0], group[1], q_lora, q_lora + kv_lora), summed(group[0], group[1], q_lora + kv_lora, q_lora + kv_lora + 128)
            else:
                ckv = halves(qh, qh + kh)
                kr = summed(group[0], group[1], qh + kh, qh + kh + 128) if mode == "pair" else group[2][src].astype(F32)
            if start >= q_lo:
                cq = summed(group[0], group[1], 0, q_lora) if mode == "full" else halves(0, qh)
                cq_ref[pl.ds(pl.multiple_of(start - q_lo + c * 128, 128), 128)] = norm(cq, gq_ref[...])
            ckv_ref[rows] = norm(ckv, gkv_ref[...])
            kk = kr * cos_ref[rows] + pltpu.roll(kr, 64, 1) * sin_ref[rows]
            odd = (lax.broadcasted_iota(jnp.int32, kk.shape, 1) // 32) % 2 == 1
            kk_ref[rows] = kk.astype(BF16)
            kpe_ref[0, rows] = jnp.where(odd, 0.0, kk).astype(BF16)
            kpe_ref[1, rows] = jnp.where(odd, kk, 0.0).astype(BF16)

    @pl.when(step == 0)
    def _():
        if mode == "sum2":
            fill(ins[:3], 0, seq // 2)
            fill(ins[3:], seq // 2, seq // 2)
        else:
            fill(ins, 0, seq)

    def nt(a, b):
        return lax.dot_general(a, b, (((1,), (1,)), ((), ())), preferred_element_type=F32)

    @pl.when(step < steps)
    def _():
        cq, ckv = cq_ref[...], ckv_ref[...]
        qn = nt(cq, wq_ref[:, :128].reshape(wide, q_lora)).astype(BF16)
        qps = []
        for pair in range(heads // 2):
            a, b = 2 * pair, 2 * pair + 1
            wr = jnp.concatenate([wq_ref[a, 128:160], wq_ref[b, 128:160], wq_ref[a, 160:192], wq_ref[b, 160:192]], axis=0)
            qr = nt(cq, wr).astype(BF16).astype(F32)
            qps.append((qr * cos_ref[q_lo:] + pltpu.roll(qr, 64, 1) * sin_ref[q_lo:]).astype(BF16))
        kn = jnp.dot(ckv, wk_ref[...], preferred_element_type=F32).astype(BF16)
        val = jnp.dot(ckv, wv_ref[...], preferred_element_type=F32).astype(BF16)
        row = lax.broadcasted_iota(jnp.int32, (blk, blk), 0)
        col = lax.broadcasted_iota(jnp.int32, (blk, blk), 1)
        allowed = col <= row
        items = [(hh, qb) for hh in range(heads) for qb in range(q_rows // blk)]

        def span(qb):
            return slice(qb * blk, (qb + 1) * blk), q_lo + (qb + 1) * blk

        def score(hh, qb):
            cols, (rows, end) = slice(hh * 128, hh * 128 + 128), span(qb)
            key = jnp.concatenate([kn[:end, cols], kpe_ref[hh % 2, :end]], axis=1)
            q = jnp.concatenate([qn[rows, cols], qps[hh // 2][rows]], axis=1)
            s = nt(q, key)
            diag = jnp.where(allowed, s[:, end - blk:], -jnp.inf)
            return diag if end == blk else jnp.concatenate([s[:, :end - blk], diag], axis=1)

        def softmax(s):
            top = jnp.max(s, axis=1, keepdims=True)
            e = jnp.exp2((s - top) * (scale * math.log2(math.e)))
            return (e * (1.0 / jnp.sum(e, axis=1, keepdims=True))).astype(BF16)

        scores = [score(*it) for it in items]
        probs = [softmax(s) for s in scores]
        for p, (hh, qb) in zip(probs, items):
            rows, end = span(qb)
            o = jnp.dot(p, val[:end, hh * 128:hh * 128 + 128], preferred_element_type=F32).astype(BF16)
            ctx_ref[rows, pl.ds(pl.multiple_of(step * wide + hh * 128, 128), 128)] = o

    @pl.when(step >= steps)
    def _():
        depth = wo_a_ref.shape[0]
        out = jnp.dot(ctx_ref[:, :depth], wo_a_ref[...], preferred_element_type=F32)
        out += jnp.dot(ctx_ref[:, depth:], wo_b_ref[...], preferred_element_type=F32)
        part_ref[...] = out.astype(BF16)


def head_block(mode, ins, at, q_lo, seq, side, gq, gkv, cos_p, sin_p, wq, wkv, wo_a, wo_b, scale):
    q_rows = seq - q_lo
    in_rows = seq // 2 if mode == "sum2" else seq
    n_heads, qk, q_lora = wq.shape
    kv_lora, depth, width = wkv.shape[0], wo_a.shape[0], wo_a.shape[1]
    heads, wide = 4, 512
    steps, out_steps = n_heads // heads, width // wide
    once = pl.Buffered(1)
    hd = lambda j: jnp.minimum(j, steps - 1)
    oc = lambda j: jnp.maximum(j - steps, 0)
    const = lambda shape: pl.BlockSpec(shape, lambda j, o: (0,) * len(shape), pipeline_mode=once)
    return pl.pallas_call(
        lambda *refs: block_kernel(scale, mode, q_lo, *refs),
        grid_spec=pltpu.PrefetchScalarGridSpec(
            num_scalar_prefetch=1,
            grid=(steps + out_steps,),
            in_specs=[pl.BlockSpec((in_rows, a.shape[1]), lambda j, o, r=r: (r, 0), pipeline_mode=once) for a, r in zip(ins, at)] + [
                const((1, q_lora)), const((1, kv_lora)), const((seq, 128)), const((seq, 128)),
                pl.BlockSpec((heads, qk, q_lora), lambda j, o: (hd(j), 0, 0)),
                pl.BlockSpec((kv_lora, wide), lambda j, o: (0, hd(j))),
                pl.BlockSpec((kv_lora, wide), lambda j, o: (0, steps + hd(j))),
                pl.BlockSpec((depth, wide), lambda j, o: (0, oc(j))),
                pl.BlockSpec((depth, wide), lambda j, o: (0, oc(j))),
            ],
            out_specs=[
                pl.BlockSpec((q_rows, wide), lambda j, o: (0, oc(j))),
                pl.BlockSpec((seq, kv_lora), lambda j, o: (0, 0)),
                pl.BlockSpec((seq, 128), lambda j, o: (0, 0)),
            ],
            scratch_shapes=[pltpu.VMEM((q_rows, q_lora), BF16), pltpu.VMEM((2, seq, 128), BF16), pltpu.VMEM((q_rows, n_heads * 128), BF16)],
        ),
        out_shape=[jax.ShapeDtypeStruct((q_rows, width), BF16), jax.ShapeDtypeStruct((seq, kv_lora), BF16), jax.ShapeDtypeStruct((seq, 128), BF16)],
        compiler_params=pltpu.CompilerParams(dimension_semantics=("arbitrary",), vmem_limit_bytes=60 * 2**20),
        cost_estimate=pl.CostEstimate(flops=45 * 10**9 * q_rows // 512, bytes_accessed=64 * 10**6, transcendentals=n_heads * seq * seq),
        name="block",
    )(side, *ins, gq, gkv, cos_p, sin_p, wq, wkv, wkv, wo_a, wo_b)


def blank(shape, dtype):
    return pl.pallas_call(lambda o_ref: None, out_shape=jax.ShapeDtypeStruct(shape, dtype), out_specs=pl.BlockSpec(memory_space=pl.ANY), name="blank")()


def solution(mesh):
    emb_count = mesh.shape["emb"]
    in_specs = (P("dp", None, "emb"), P("emb"), P("emb", "head"), P("head"), P("emb", "head"), P("head"), P("emb", None), P(None, "head", None), P(None, "head", None), P(None, "head", None), P("head", None, "emb"))
    out_specs = (P("dp", None, "emb"), P("dp", None, "head"), P("dp", None, None))

    def swap(v):
        return lax.ppermute(v, "head", SIBLING)

    def cross(v):
        return lax.ppermute(v, "head", ACROSS)

    def emb_swap(v):
        return lax.ppermute(v, "emb", EMB_SWAP)

    def block(hidden, g_in, w_dq, g_q, w_dkv, g_kv, w_kr, w_uq, w_uk, w_uv, w_o):
        n_seq, seq, width = hidden.shape
        half = n_seq // 2
        own_heads = w_uk.shape[1]
        q_lora, kv_lora = w_uq.shape[0], w_uk.shape[0]
        q_blk, kv_blk = w_dq.shape[1], w_dkv.shape[1]
        rope = w_kr.shape[1]
        hr = rope // 2
        scale = MSCALE * MSCALE / math.sqrt(w_uq.shape[2])
        pos = lax.axis_index("head")
        core = lax.rem(pos, 2)
        side = lax.div(pos, 2)
        base = core * half

        far_q = cross(w_dq)
        far_kv = cross(w_dkv)
        near_q, near_kv = swap(w_dq), swap(w_dkv)
        sib_uq, sib_uk, sib_uv = swap(w_uq), swap(w_uk), swap(w_uv)
        sib_o = swap(w_o)

        cos_p, sin_p = rope_tables(seq, rope)
        w_kr2 = jnp.concatenate([w_kr[:, :hr], w_kr[:, :hr], w_kr[:, hr:], w_kr[:, hr:]], axis=1)
        gain = jnp.concatenate([g_q, g_kv])[None]
        far_gain = cross(gain)
        g_row = g_in.astype(F32)[None]

        h_wide = lax.dynamic_slice_in_dim(hidden, base, half, 0).astype(F32)
        sq = jnp.sum(h_wide * h_wide, axis=-1)
        sq = sq + emb_swap(sq)
        rstd = lax.rsqrt(sq / (width * emb_count) + NORM_EPS)[:, :, None]

        qh, kh = 2 * q_blk, 2 * kv_blk
        near_offs = [core * q_blk, (1 - core) * q_blk, qh + core * kv_blk, qh + (1 - core) * kv_blk]
        low_own = down(hidden, rstd, g_row, 0, FIRST, base, [w_dq, near_q, w_dkv, near_kv, w_kr2], near_offs + [qh + kh])

        def rows_of(low, r):
            return low[r * seq:(r + 1) * seq]

        cuts = [(0, seq // 2), (seq // 2, seq)] + [(r * seq, r * seq + seq) for r in range(1, FIRST)]
        own_in = [emb_swap(low_own[lo:hi]) for lo, hi in cuts]

        w_uq, sib_uq, w_uk, w_uv, sib_uk, sib_uv = after((w_uq, sib_uq, w_uk, w_uv, sib_uk, sib_uv), low_own)
        flat = lambda w: w.reshape(kv_lora, own_heads * 128)
        wkv_all = jnp.concatenate([flat(w_uk), flat(sib_uk), flat(w_uv), flat(sib_uv)], axis=1)
        wq_all = jnp.concatenate([w_uq.transpose(1, 2, 0), after(sib_uq, wkv_all).transpose(1, 2, 0)], axis=0)
        wo_own, wo_sib = w_o.reshape(own_heads * 128, width), sib_o.reshape(own_heads * 128, width)

        lats = []
        for k, (lo, hi) in enumerate(cuts[:2]):
            got = own_in[k] if k == 0 else after(own_in[k], lat)
            lat = (low_own[lo:hi].astype(F32) + got.astype(F32)).astype(BF16)
            far_lat = cross(lat[:, :qh + kh])
            lats.append((lat[:, :qh + kh], far_lat, lat[:, qh + kh:]))
        low_x = cross(low_own[seq:2 * seq, :qh + kh])
        far_gain, far_q = after((far_gain, far_q), wq_all, wkv_all)
        gains = jnp.concatenate([gain, swap(gain), far_gain, swap(far_gain)], axis=0).astype(F32)
        gains = jnp.concatenate([lax.dynamic_slice_in_dim(gains, lax.bitwise_xor(pos, r), 1, 0) for r in range(4)], axis=0)
        gq_all = gains[:, :q_blk].reshape(1, q_lora)
        gkv_all = gains[:, q_blk:].reshape(1, kv_lora)
        diag_q = swap(far_q)
        every_offs = [lax.bitwise_xor(pos, r) * q_blk for r in range(4)] + [q_lora + lax.bitwise_xor(pos, r) * kv_blk for r in range(4)] + [q_lora + kv_lora]

        side_flag = side.astype(jnp.int32)[None]
        parts, arrived, ckvs, kks = {}, {}, [], []
        last = wq_all
        result = blank(hidden.shape, BF16)

        def finish(i, lo, hi, dep):
            at = after(base, *dep)
            h_i = lax.dynamic_slice(hidden, (at + i, 0 * at + lo, 0 * at), (1, hi - lo, width)).astype(F32)
            total = parts[i, lo].astype(F32) + arrived[i, lo].astype(F32)
            return (h_i + total[None]).astype(BF16)

        def run(mode, ins, at, q_lo, rows, dep):
            return head_block(mode, ins, at, q_lo, rows, side_flag, after(gq_all, dep), gkv_all, cos_p, sin_p, wq_all, wkv_all, wo_own, wo_sib, scale)

        def send(i, lo, part):
            parts[i, lo] = part
            arrived[i, lo] = cross(part)

        hs = seq // 2
        part_a, _, _ = run("sum", lats[0], (0,) * 3, 0, hs, last)
        send(0, 0, part_a)
        low_xy = emb_swap(after(low_x, part_a))
        part, ckv, kk = run("sum2", lats[0] + lats[1], (0,) * 6, hs, seq, part_a)
        send(0, hs, part)
        ckvs.append(ckv)
        kks.append(kk)
        far_kv = after(far_kv, part)
        diag_kv = swap(far_kv)
        every = [w_dq, near_q, far_q, diag_q, w_dkv, near_kv, far_kv, diag_kv, w_kr2]
        lows = {1: ("pair", (low_own, own_in[2], low_x, low_xy), (1, 0, 0, 0))}
        last = part
        for i in range(1, half):
            mode, ins, at = lows[i]
            part, ckv, kk = run(mode, ins, at, 0, seq, last)
            ckvs.append(ckv)
            kks.append(kk)
            last = part
            for lo, hi in PIECES.get(i, ((0, seq),)):
                send(i, lo, part[lo:hi])
            if i == 1:
                last = down(hidden, after(rstd, last), g_row, 2, 1, base, [far_q, diag_q, far_kv, diag_kv], near_offs)
                lows[2] = ("pair", (low_own, own_in[3], last, emb_swap(last)), (2, 0, 0, 0))
            for first, n in DOWNS.get(i, ()):
                low = down(hidden, after(rstd, last), g_row, first, n, base, every, every_offs)
                last = low
                for r in range(n):
                    lows[first + r] = ("full", (low, emb_swap(rows_of(low, r))), (r, 0))

        def spread(own, other):
            full = blank((n_seq,) + own.shape[1:], own.dtype)
            full = lax.dynamic_update_slice_in_dim(full, own, base, 0)
            return lax.dynamic_update_slice_in_dim(full, other, half - base, 0)

        ckv_own = jnp.concatenate(ckvs, axis=0).reshape(half, seq, kv_lora)
        kk = jnp.concatenate(kks, axis=0)
        kk = jnp.concatenate([kk[:, :hr], kk[:, 2 * hr:3 * hr]], axis=1).reshape(half, seq, rope)
        mine = lax.dynamic_slice_in_dim(ckv_own, pos * kv_blk, kv_blk, 2)
        theirs = lax.dynamic_slice_in_dim(ckv_own, lax.bitwise_xor(pos, 1) * kv_blk, kv_blk, 2)
        ckv_out, kpe_out = spread(mine, swap(theirs)), spread(kk, swap(kk))

        waiting = []

        def place(result):
            i, lo, other = waiting.pop(0)
            return lax.dynamic_update_slice(result, other, (half - base + i, 0 * base + lo, 0 * base))

        for i in range(half):
            for lo, hi in PIECES.get(i, ((0, seq),)):
                out_i = finish(i, lo, hi, (last,))
                waiting.append((i, lo, swap(out_i)))
                result = lax.dynamic_update_slice(result, out_i, (base + i, 0 * base + lo, 0 * base))
                if len(waiting) > 1:
                    result = place(result)
        result = place(result)
        return result, ckv_out, kpe_out

    return jax.shard_map(block, mesh=mesh, in_specs=in_specs, out_specs=out_specs, check_vma=False)
```

```python
import math
import jax
import jax.numpy as jnp
from jax import lax
from jax.experimental import pallas as pl
from jax.experimental.pallas import tpu as pltpu
from jax.sharding import PartitionSpec as P

ROPE_BASE = 10000.0
NORM_EPS = 1.0e-6
MSCALE = 0.1 * math.log(40.0) + 1.0
BF16 = jnp.bfloat16
F32 = jnp.float32


SIBLING = [(0, 1), (1, 0), (2, 3), (3, 2)]
ACROSS = [(0, 2), (2, 0), (1, 3), (3, 1)]
EMB_SWAP = [(0, 1), (1, 0)]

FIRST = 3
DOWNS = {1: ((3, 1),), 2: ((4, 1),), 3: ((5, 3),)}
PIECES = {0: ((0, 256), (256, 512)), 7: ((0, 384), (384, 512))}
ROWS = 256


def after(value, *deps):
    return lax.optimization_barrier((value,) + deps)[0]


def rope_tables(seq_len, rope_dim):
    half_dim = rope_dim // 2
    inv_freq = ROPE_BASE ** (-2.0 * jnp.arange(half_dim, dtype=F32) / rope_dim)
    angles = jnp.arange(seq_len, dtype=F32)[:, None] * inv_freq[None, :]
    cos_t, sin_t = jnp.cos(angles), jnp.sin(angles)
    return jnp.concatenate([cos_t] * 4, axis=1), jnp.concatenate([-sin_t, -sin_t, sin_t, sin_t], axis=1)


def down_kernel(offs_ref, h_ref, rstd_ref, g_ref, *rest):
    pieces, out_ref, w_all = rest[:-2], rest[-2], rest[-1]

    @pl.when(pl.program_id(0) == 0)
    def _():
        for k, ref in enumerate(pieces):
            off = pl.multiple_of(offs_ref[k + 1], 128)
            w_all[:, pl.ds(off, ref.shape[1])] = ref[...]

    hn = (h_ref[0].astype(F32) * rstd_ref[0] * g_ref[...]).astype(BF16)
    out_ref[...] = jnp.dot(hn, w_all[...], preferred_element_type=F32).astype(BF16)


def down(hidden, rstd, g_in, first, n, core_base, pieces, offsets):
    seq, width = hidden.shape[1:]
    tiles = seq // ROWS
    total = sum(p.shape[1] for p in pieces)
    offs = jnp.stack([core_base + first] + [jnp.asarray(o, jnp.int32) for o in offsets]).astype(jnp.int32)
    whole = lambda p: pl.BlockSpec(p.shape, lambda t, o: (0, 0), pipeline_mode=pl.Buffered(1))
    return pl.pallas_call(
        down_kernel,
        grid_spec=pltpu.PrefetchScalarGridSpec(
            num_scalar_prefetch=1,
            grid=(n * tiles,),
            in_specs=[
                pl.BlockSpec((1, ROWS, width), lambda t, o: (o[0] + t // tiles, t % tiles, 0)),
                pl.BlockSpec((1, ROWS, 1), lambda t, o: (first + t // tiles, t % tiles, 0)),
                whole(g_in),
            ] + [whole(p) for p in pieces],
            out_specs=pl.BlockSpec((ROWS, total), lambda t, o: (t, 0)),
            scratch_shapes=[pltpu.VMEM((width, total), BF16)],
        ),
        out_shape=jax.ShapeDtypeStruct((n * seq, total), BF16),
        compiler_params=pltpu.CompilerParams(dimension_semantics=("arbitrary",)),
        cost_estimate=pl.CostEstimate(flops=2 * n * seq * width * total, bytes_accessed=2 * n * seq * width + 2 * width * total, transcendentals=0),
        name="down",
    )(offs, hidden, rstd, g_in, *pieces)


def block_kernel(scale, mode, q_lo, side_ref, *refs):
    n_in = {"full": 2, "pair": 4, "sum": 3, "sum2": 6}[mode]
    ins = refs[:n_in]
    gq_ref, gkv_ref, cos_ref, sin_ref, wq_ref, wk_ref, wv_ref, wo_a_ref, wo_b_ref = refs[n_in:n_in + 9]
    part_ref, ckv_ref, kk_ref, cq_ref, kpe_ref, ctx_ref = refs[n_in + 9:]
    step = pl.program_id(0)
    q_rows, q_lora = cq_ref.shape
    seq, kv_lora = ckv_ref.shape
    heads = wq_ref.shape[0]
    wide = heads * 128
    steps = ctx_ref.shape[1] // wide
    blk = 256
    qh, kh = q_lora // 2, kv_lora // 2

    def norm(vals, gain):
        mean_sq = jnp.mean(vals * vals, axis=-1, keepdims=True)
        return (vals * lax.rsqrt(mean_sq + NORM_EPS) * gain).astype(BF16)

    def fill(group, start, count):
        @pl.loop(0, count // 128)
        def _(c):
            src = pl.ds(pl.multiple_of(c * 128, 128), 128)
            rows = pl.ds(pl.multiple_of(start + c * 128, 128), 128)

            def summed(a_ref, b_ref, lo, hi):
                return (a_ref[src, lo:hi].astype(F32) + b_ref[src, lo:hi].astype(F32)).astype(BF16).astype(F32)

            def halves(lo, hi):
                if mode == "pair":
                    own, far = summed(group[0], group[1], lo, hi), summed(group[2], group[3], lo, hi)
                else:
                    own, far = group[0][src, lo:hi].astype(F32), group[1][src, lo:hi].astype(F32)
                first = side_ref[0] == 0
                return jnp.concatenate([jnp.where(first, own, far), jnp.where(first, far, own)], axis=1)

            if mode == "full":
                ckv, kr = summed(group[0], group[1], q_lora, q_lora + kv_lora), summed(group[0], group[1], q_lora + kv_lora, q_lora + kv_lora + 128)
            else:
                ckv = halves(qh, qh + kh)
                kr = summed(group[0], group[1], qh + kh, qh + kh + 128) if mode == "pair" else group[2][src].astype(F32)
            if start >= q_lo:
                cq = summed(group[0], group[1], 0, q_lora) if mode == "full" else halves(0, qh)
                cq_ref[pl.ds(pl.multiple_of(start - q_lo + c * 128, 128), 128)] = norm(cq, gq_ref[...])
            ckv_ref[rows] = norm(ckv, gkv_ref[...])
            kk = kr * cos_ref[rows] + pltpu.roll(kr, 64, 1) * sin_ref[rows]
            odd = (lax.broadcasted_iota(jnp.int32, kk.shape, 1) // 32) % 2 == 1
            kk_ref[rows] = kk.astype(BF16)
            kpe_ref[0, rows] = jnp.where(odd, 0.0, kk).astype(BF16)
            kpe_ref[1, rows] = jnp.where(odd, kk, 0.0).astype(BF16)

    @pl.when(step == 0)
    def _():
        if mode == "sum2":
            fill(ins[:3], 0, seq // 2)
            fill(ins[3:], seq // 2, seq // 2)
        else:
            fill(ins, 0, seq)

    def nt(a, b):
        return lax.dot_general(a, b, (((1,), (1,)), ((), ())), preferred_element_type=F32)

    @pl.when(step < steps)
    def _():
        cq, ckv = cq_ref[...], ckv_ref[...]
        qn = nt(cq, wq_ref[:, :128].reshape(wide, q_lora)).astype(BF16)
        qps = []
        for pair in range(heads // 2):
            a, b = 2 * pair, 2 * pair + 1
            wr = jnp.concatenate([wq_ref[a, 128:160], wq_ref[b, 128:160], wq_ref[a, 160:192], wq_ref[b, 160:192]], axis=0)
            qr = nt(cq, wr).astype(BF16).astype(F32)
            qps.append((qr * cos_ref[q_lo:] + pltpu.roll(qr, 64, 1) * sin_ref[q_lo:]).astype(BF16))
        kn = jnp.dot(ckv, wk_ref[...], preferred_element_type=F32).astype(BF16)
        val = jnp.dot(ckv, wv_ref[...], preferred_element_type=F32).astype(BF16)
        row = lax.broadcasted_iota(jnp.int32, (blk, blk), 0)
        col = lax.broadcasted_iota(jnp.int32, (blk, blk), 1)
        allowed = col <= row
        items = [(hh, qb) for hh in range(heads) for qb in range(q_rows // blk)]

        def span(qb):
            return slice(qb * blk, (qb + 1) * blk), q_lo + (qb + 1) * blk

        def score(hh, qb):
            cols, (rows, end) = slice(hh * 128, hh * 128 + 128), span(qb)
            key = jnp.concatenate([kn[:end, cols], kpe_ref[hh % 2, :end]], axis=1)
            q = jnp.concatenate([qn[rows, cols], qps[hh // 2][rows]], axis=1)
            s = nt(q, key)
            diag = jnp.where(allowed, s[:, end - blk:], -jnp.inf)
            return diag if end == blk else jnp.concatenate([s[:, :end - blk], diag], axis=1)

        def softmax(s):
            top = jnp.max(s, axis=1, keepdims=True)
            e = jnp.exp2((s - top) * (scale * math.log2(math.e)))
            return (e * (1.0 / jnp.sum(e, axis=1, keepdims=True))).astype(BF16)

        scores = [score(*it) for it in items]
        probs = [softmax(s) for s in scores]
        for p, (hh, qb) in zip(probs, items):
            rows, end = span(qb)
            o = jnp.dot(p, val[:end, hh * 128:hh * 128 + 128], preferred_element_type=F32).astype(BF16)
            ctx_ref[rows, pl.ds(pl.multiple_of(step * wide + hh * 128, 128), 128)] = o

    @pl.when(step >= steps)
    def _():
        depth = wo_a_ref.shape[0]
        out = jnp.dot(ctx_ref[:, :depth], wo_a_ref[...], preferred_element_type=F32)
        out += jnp.dot(ctx_ref[:, depth:], wo_b_ref[...], preferred_element_type=F32)
        part_ref[...] = out.astype(BF16)


def head_block(mode, ins, at, q_lo, seq, side, gq, gkv, cos_p, sin_p, wq, wkv, wo_a, wo_b, scale):
    q_rows = seq - q_lo
    in_rows = seq // 2 if mode == "sum2" else seq
    n_heads, qk, q_lora = wq.shape
    kv_lora, depth, width = wkv.shape[0], wo_a.shape[0], wo_a.shape[1]
    heads, wide, cols = 8, 1024, 512
    steps, out_steps = n_heads // heads, width // cols
    once = pl.Buffered(1)
    hd = lambda j: jnp.minimum(j, steps - 1)
    oc = lambda j: jnp.maximum(j - steps, 0)
    const = lambda shape: pl.BlockSpec(shape, lambda j, o: (0,) * len(shape), pipeline_mode=once)
    return pl.pallas_call(
        lambda *refs: block_kernel(scale, mode, q_lo, *refs),
        grid_spec=pltpu.PrefetchScalarGridSpec(
            num_scalar_prefetch=1,
            grid=(steps + out_steps,),
            in_specs=[pl.BlockSpec((in_rows, a.shape[1]), lambda j, o, r=r: (r, 0), pipeline_mode=once) for a, r in zip(ins, at)] + [
                const((1, q_lora)), const((1, kv_lora)), const((seq, 128)), const((seq, 128)),
                pl.BlockSpec((heads, qk, q_lora), lambda j, o: (hd(j), 0, 0)),
                pl.BlockSpec((kv_lora, wide), lambda j, o: (0, hd(j))),
                pl.BlockSpec((kv_lora, wide), lambda j, o: (0, steps + hd(j))),
                pl.BlockSpec((depth, cols), lambda j, o: (0, oc(j))),
                pl.BlockSpec((depth, cols), lambda j, o: (0, oc(j))),
            ],
            out_specs=[
                pl.BlockSpec((q_rows, cols), lambda j, o: (0, oc(j))),
                pl.BlockSpec((seq, kv_lora), lambda j, o: (0, 0)),
                pl.BlockSpec((seq, 128), lambda j, o: (0, 0)),
            ],
            scratch_shapes=[pltpu.VMEM((q_rows, q_lora), BF16), pltpu.VMEM((2, seq, 128), BF16), pltpu.VMEM((q_rows, n_heads * 128), BF16)],
        ),
        out_shape=[jax.ShapeDtypeStruct((q_rows, width), BF16), jax.ShapeDtypeStruct((seq, kv_lora), BF16), jax.ShapeDtypeStruct((seq, 128), BF16)],
        compiler_params=pltpu.CompilerParams(dimension_semantics=("arbitrary",), vmem_limit_bytes=60 * 2**20),
        cost_estimate=pl.CostEstimate(flops=45 * 10**9 * q_rows // 512, bytes_accessed=64 * 10**6, transcendentals=n_heads * seq * seq),
        name="block",
    )(side, *ins, gq, gkv, cos_p, sin_p, wq, wkv, wkv, wo_a, wo_b)


def blank(shape, dtype):
    return pl.pallas_call(lambda o_ref: None, out_shape=jax.ShapeDtypeStruct(shape, dtype), out_specs=pl.BlockSpec(memory_space=pl.ANY), name="blank")()


def solution(mesh):
    emb_count = mesh.shape["emb"]
    in_specs = (P("dp", None, "emb"), P("emb"), P("emb", "head"), P("head"), P("emb", "head"), P("head"), P("emb", None), P(None, "head", None), P(None, "head", None), P(None, "head", None), P("head", None, "emb"))
    out_specs = (P("dp", None, "emb"), P("dp", None, "head"), P("dp", None, None))

    def swap(v):
        return lax.ppermute(v, "head", SIBLING)

    def cross(v):
        return lax.ppermute(v, "head", ACROSS)

    def emb_swap(v):
        return lax.ppermute(v, "emb", EMB_SWAP)

    def block(hidden, g_in, w_dq, g_q, w_dkv, g_kv, w_kr, w_uq, w_uk, w_uv, w_o):
        n_seq, seq, width = hidden.shape
        half = n_seq // 2
        own_heads = w_uk.shape[1]
        q_lora, kv_lora = w_uq.shape[0], w_uk.shape[0]
        q_blk, kv_blk = w_dq.shape[1], w_dkv.shape[1]
        rope = w_kr.shape[1]
        hr = rope // 2
        scale = MSCALE * MSCALE / math.sqrt(w_uq.shape[2])
        pos = lax.axis_index("head")
        core = lax.rem(pos, 2)
        side = lax.div(pos, 2)
        base = core * half

        far_q = cross(w_dq)
        far_kv = cross(w_dkv)
        near_q, near_kv = swap(w_dq), swap(w_dkv)
        sib_uq, sib_uk, sib_uv = swap(w_uq), swap(w_uk), swap(w_uv)
        sib_o = swap(w_o)

        cos_p, sin_p = rope_tables(seq, rope)
        w_kr2 = jnp.concatenate([w_kr[:, :hr], w_kr[:, :hr], w_kr[:, hr:], w_kr[:, hr:]], axis=1)
        gain = jnp.concatenate([g_q, g_kv])[None]
        far_gain = cross(gain)
        g_row = g_in.astype(F32)[None]

        h_wide = lax.dynamic_slice_in_dim(hidden, base, half, 0).astype(F32)
        sq = jnp.sum(h_wide * h_wide, axis=-1)
        sq = sq + emb_swap(sq)
        rstd = lax.rsqrt(sq / (width * emb_count) + NORM_EPS)[:, :, None]

        qh, kh = 2 * q_blk, 2 * kv_blk
        near_offs = [core * q_blk, (1 - core) * q_blk, qh + core * kv_blk, qh + (1 - core) * kv_blk]
        low_own = down(hidden, rstd, g_row, 0, FIRST, base, [w_dq, near_q, w_dkv, near_kv, w_kr2], near_offs + [qh + kh])

        def rows_of(low, r):
            return low[r * seq:(r + 1) * seq]

        cuts = [(0, seq // 2), (seq // 2, seq)] + [(r * seq, r * seq + seq) for r in range(1, FIRST)]
        own_in = [emb_swap(low_own[lo:hi]) for lo, hi in cuts]

        w_uq, sib_uq, w_uk, w_uv, sib_uk, sib_uv = after((w_uq, sib_uq, w_uk, w_uv, sib_uk, sib_uv), low_own)
        flat = lambda w: w.reshape(kv_lora, own_heads * 128)
        wkv_all = jnp.concatenate([flat(w_uk), flat(sib_uk), flat(w_uv), flat(sib_uv)], axis=1)
        wq_all = jnp.concatenate([w_uq.transpose(1, 2, 0), after(sib_uq, wkv_all).transpose(1, 2, 0)], axis=0)
        wo_own, wo_sib = w_o.reshape(own_heads * 128, width), sib_o.reshape(own_heads * 128, width)

        lats = []
        for k, (lo, hi) in enumerate(cuts[:2]):
            got = own_in[k] if k == 0 else after(own_in[k], lat)
            lat = (low_own[lo:hi].astype(F32) + got.astype(F32)).astype(BF16)
            far_lat = cross(lat[:, :qh + kh])
            lats.append((lat[:, :qh + kh], far_lat, lat[:, qh + kh:]))
        low_x = cross(low_own[seq:2 * seq, :qh + kh])
        far_gain, far_q = after((far_gain, far_q), wq_all, wkv_all)
        gains = jnp.concatenate([gain, swap(gain), far_gain, swap(far_gain)], axis=0).astype(F32)
        gains = jnp.concatenate([lax.dynamic_slice_in_dim(gains, lax.bitwise_xor(pos, r), 1, 0) for r in range(4)], axis=0)
        gq_all = gains[:, :q_blk].reshape(1, q_lora)
        gkv_all = gains[:, q_blk:].reshape(1, kv_lora)
        diag_q = swap(far_q)
        every_offs = [lax.bitwise_xor(pos, r) * q_blk for r in range(4)] + [q_lora + lax.bitwise_xor(pos, r) * kv_blk for r in range(4)] + [q_lora + kv_lora]

        side_flag = side.astype(jnp.int32)[None]
        parts, arrived, ckvs, kks = {}, {}, [], []
        last = wq_all
        result = blank(hidden.shape, BF16)

        def finish(i, lo, hi, dep):
            at = after(base, *dep)
            h_i = lax.dynamic_slice(hidden, (at + i, 0 * at + lo, 0 * at), (1, hi - lo, width)).astype(F32)
            total = parts[i, lo].astype(F32) + arrived[i, lo].astype(F32)
            return (h_i + total[None]).astype(BF16)

        def run(mode, ins, at, q_lo, rows, dep):
            return head_block(mode, ins, at, q_lo, rows, side_flag, after(gq_all, dep), gkv_all, cos_p, sin_p, wq_all, wkv_all, wo_own, wo_sib, scale)

        def send(i, lo, part):
            parts[i, lo] = part
            arrived[i, lo] = cross(part)

        hs = seq // 2
        part_a, _, _ = run("sum", lats[0], (0,) * 3, 0, hs, last)
        send(0, 0, part_a)
        low_xy = emb_swap(after(low_x, part_a))
        part, ckv, kk = run("sum2", lats[0] + lats[1], (0,) * 6, hs, seq, part_a)
        send(0, hs, part)
        ckvs.append(ckv)
        kks.append(kk)
        far_kv = after(far_kv, part_a)
        diag_kv = swap(far_kv)
        every = [w_dq, near_q, far_q, diag_q, w_dkv, near_kv, far_kv, diag_kv, w_kr2]
        lows = {1: ("pair", (low_own, own_in[2], low_x, low_xy), (1, 0, 0, 0))}
        last = part
        last = down(hidden, rstd, g_row, 2, 1, after(base, last), [far_q, diag_q, far_kv, diag_kv], near_offs)
        lows[2] = ("pair", (low_own, own_in[3], last, emb_swap(last)), (2, 0, 0, 0))
        for i in range(1, half):
            mode, ins, at = lows[i]
            part, ckv, kk = run(mode, ins, at, 0, seq, last)
            ckvs.append(ckv)
            kks.append(kk)
            last = part
            for lo, hi in PIECES.get(i, ((0, seq),)):
                send(i, lo, part[lo:hi])
            for first, n in DOWNS.get(i, ()):
                low = down(hidden, rstd, g_row, first, n, after(base, last), every, every_offs)
                last = low
                for r in range(n):
                    lows[first + r] = ("full", (low, emb_swap(rows_of(low, r))), (r, 0))

        def spread(own, other):
            full = blank((n_seq,) + own.shape[1:], own.dtype)
            full = lax.dynamic_update_slice_in_dim(full, own, base, 0)
            return lax.dynamic_update_slice_in_dim(full, other, half - base, 0)

        ckv_own = jnp.concatenate(ckvs, axis=0).reshape(half, seq, kv_lora)
        kk = jnp.concatenate(kks, axis=0)
        kk = jnp.concatenate([kk[:, :hr], kk[:, 2 * hr:3 * hr]], axis=1).reshape(half, seq, rope)
        mine = lax.dynamic_slice_in_dim(ckv_own, pos * kv_blk, kv_blk, 2)
        theirs = lax.dynamic_slice_in_dim(ckv_own, lax.bitwise_xor(pos, 1) * kv_blk, kv_blk, 2)
        ckv_out, kpe_out = spread(mine, swap(theirs)), spread(kk, swap(kk))

        waiting = []

        def place(result):
            i, lo, other = waiting.pop(0)
            return lax.dynamic_update_slice(result, other, (half - base + i, 0 * base + lo, 0 * base))

        for i in range(half):
            for lo, hi in PIECES.get(i, ((0, seq),)):
                out_i = finish(i, lo, hi, (last,))
                waiting.append((i, lo, swap(out_i)))
                result = lax.dynamic_update_slice(result, out_i, (base + i, 0 * base + lo, 0 * base))
                if len(waiting) > 1:
                    result = place(result)
        result = place(result)
        return result, ckv_out, kpe_out

    return jax.shard_map(block, mesh=mesh, in_specs=in_specs, out_specs=out_specs, check_vma=False)
```
